16 devices in a mesh: dp: 2 (over y, z), tp: 8 (over x, core).
Axes of the slice: x: 4, y: 2, z: 1, core: 2. Of those that a mesh axis runs over, the one named last changes fastest.
The devices are a block of a 4x4x8 slice.
Arguments:
- x_in: bfloat16 [24, 1024, 2048], P('dp'), parts along dimension 0
- seq_lens: int32 [24], P('dp'), parts along dimension 0
- ln1_gain: float32 [2048], replicated
- ln1_bias: float32 [2048], replicated
- w_qkv: bfloat16 [2048, 3, 32, 64], P(None, None, 'tp')
- b_qkv: bfloat16 [3, 32, 64], P(None, 'tp')
- w_out: bfloat16 [32, 64, 2048], P('tp')
- b_out: bfloat16 [2048], replicated
- ln2_gain: float32 [2048], replicated
- ln2_bias: float32 [2048], replicated
- w_up: bfloat16 [2048, 8192], P(None, 'tp')
- b_up: bfloat16 [8192], P('tp')
- w_down: bfloat16 [8192, 2048], P('tp')
- b_down: bfloat16 [2048], replicated
Outputs:
- output 1: bfloat16 [24, 1024, 2048], P('dp'), parts along dimension 0
- output 2: bfloat16 [24, 32, 1024, 64], P('dp', 'tp'), parts along dimension 0
- output 3: bfloat16 [24, 32, 1024, 64], P('dp', 'tp'), parts along dimension 0
There are 2 independent parts. The reference program is written for one: setup_inputs(seed, part) draws one part's arguments, and reference() takes and returns one part's arrays. A program takes and returns all parts, laid end to end along the dimension named above; an argument that names none is the same for every part.
All inputs are finite; a program needn't handle non-finite values.
Results may differ from the reference program's by a relative error of at most 0.0134191.
Values are sent between devices in bfloat16 or wider.
A program may use at most 768 MiB of HBM per device.

```python
import jax
import jax.numpy as jnp
from jax import lax

D = 2048
HEADS = 32
HEAD = 64
BATCH = 12
SEQ = 1024
FF = 4 * D
MIN_LEN = SEQ // 8


def setup_inputs(seed: int = 0, part: int = 0) -> dict:
    base_key = jax.random.key(seed)
    weight_keys = jax.random.split(base_key, 12)
    part_key = jax.random.fold_in(base_key, part)
    act_key, len_key = jax.random.split(part_key, 2)
    x_in = jax.random.normal(act_key, (BATCH, SEQ, D), jnp.float32).astype(jnp.bfloat16)
    seq_lens = jax.random.randint(len_key, (BATCH,), MIN_LEN, SEQ, jnp.int32).at[0].set(SEQ)
    return {
        "x_in": x_in,
        "seq_lens": seq_lens,
        "ln1_gain": 1.0 + 0.3 * jax.random.normal(weight_keys[0], (D,), jnp.float32),
        "ln1_bias": 0.3 * jax.random.normal(weight_keys[1], (D,), jnp.float32),
        "w_qkv": (1.5 * D ** -0.5 * jax.random.normal(weight_keys[2], (D, 3, HEADS, HEAD), jnp.float32)).astype(jnp.bfloat16),
        "b_qkv": (0.5 * jax.random.normal(weight_keys[3], (3, HEADS, HEAD), jnp.float32)).astype(jnp.bfloat16),
        "w_out": ((HEADS * HEAD) ** -0.5 * jax.random.normal(weight_keys[4], (HEADS, HEAD, D), jnp.float32)).astype(jnp.bfloat16),
        "b_out": (0.5 * jax.random.normal(weight_keys[5], (D,), jnp.float32)).astype(jnp.bfloat16),
        "ln2_gain": 1.0 + 0.3 * jax.random.normal(weight_keys[6], (D,), jnp.float32),
        "ln2_bias": 0.3 * jax.random.normal(weight_keys[7], (D,), jnp.float32),
        "w_up": (D ** -0.5 * jax.random.normal(weight_keys[8], (D, FF), jnp.float32)).astype(jnp.bfloat16),
        "b_up": (0.5 * jax.random.normal(weight_keys[9], (FF,), jnp.float32)).astype(jnp.bfloat16),
        "w_down": (FF ** -0.5 * jax.random.normal(weight_keys[10], (FF, D), jnp.float32)).astype(jnp.bfloat16),
        "b_down": (0.5 * jax.random.normal(weight_keys[11], (D,), jnp.float32)).astype(jnp.bfloat16),
    }


def layer_norm(values, gain_vec, bias_vec):
    values = values.astype(jnp.float32)
    row_mean = jnp.mean(values, axis=-1, keepdims=True)
    centered = values - row_mean
    row_var = jnp.mean(centered * centered, axis=-1, keepdims=True)
    return (centered * lax.rsqrt(row_var + 1e-5) * gain_vec + bias_vec).astype(jnp.bfloat16)


def cache_keep(values, seq_lens):
    positions = jnp.arange(SEQ)
    valid = positions[None, None, :, None] < seq_lens[:, None, None, None]
    return jnp.where(valid, values, 0)


def attend_one(item):
    q_head, k_head, v_head, length = item
    positions = jnp.arange(SEQ)
    allowed = (positions[None, :] <= positions[:, None]) & (positions[None, :] < length)
    scores = jnp.dot(q_head, k_head.T, preferred_element_type=jnp.float32) * HEAD ** -0.5
    scores = jnp.where(allowed, scores, -1e30)
    attn_probs = jax.nn.softmax(scores, axis=-1).astype(jnp.bfloat16)
    return jnp.dot(attn_probs, v_head, preferred_element_type=jnp.float32).astype(jnp.bfloat16)


def reference(x_in, seq_lens, ln1_gain, ln1_bias, w_qkv, b_qkv, w_out, b_out, ln2_gain, ln2_bias, w_up, b_up, w_down, b_down):
    tok_count = BATCH * SEQ
    inner_width = 3 * HEADS * HEAD
    normed = layer_norm(x_in.reshape(tok_count, D), ln1_gain, ln1_bias)
    qkv_flat = jnp.dot(normed, w_qkv.reshape(D, inner_width), preferred_element_type=jnp.float32)
    qkv_flat = (qkv_flat + b_qkv.reshape(inner_width).astype(jnp.float32)).astype(jnp.bfloat16)
    qkv_all = jnp.transpose(qkv_flat.reshape(BATCH, SEQ, 3, HEADS, HEAD), (2, 0, 3, 1, 4))
    q_all = qkv_all[0]
    k_all = qkv_all[1]
    v_all = qkv_all[2]
    pair_count = BATCH * HEADS
    head_lens = jnp.repeat(seq_lens, HEADS)
    attended = lax.map(attend_one, (q_all.reshape(pair_count, SEQ, HEAD), k_all.reshape(pair_count, SEQ, HEAD), v_all.reshape(pair_count, SEQ, HEAD), head_lens))
    attended = attended.reshape(BATCH, HEADS, SEQ, HEAD)
    out_proj = jnp.einsum("bhsk,hkd->bsd", attended.astype(jnp.float32), w_out.astype(jnp.float32))
    x_mid = (x_in.astype(jnp.float32) + out_proj + b_out.astype(jnp.float32)).astype(jnp.bfloat16)
    normed2 = layer_norm(x_mid.reshape(tok_count, D), ln2_gain, ln2_bias)
    up_proj = jnp.dot(normed2, w_up, preferred_element_type=jnp.float32) + b_up.astype(jnp.float32)
    hidden = jax.nn.relu(up_proj).astype(jnp.bfloat16)
    down_proj = jnp.dot(hidden, w_down, preferred_element_type=jnp.float32) + b_down.astype(jnp.float32)
    x_out = (x_mid.reshape(tok_count, D).astype(jnp.float32) + down_proj).astype(jnp.bfloat16)
    return (x_out.reshape(BATCH, SEQ, D), cache_keep(k_all, seq_lens), cache_keep(v_all, seq_lens))
```

```python
import functools
import math

import jax
import jax.numpy as jnp
from jax import lax
from jax.experimental import pallas as pl
from jax.experimental.pallas import tpu as pltpu
from jax.sharding import PartitionSpec as P

F32 = jnp.float32
BF16 = jnp.bfloat16
NT = (((1,), (1,)), ((), ()))

def k1_body(hd, lens_ref, x_ref, g_ref, bt_ref, wt_ref, bq_ref, bkv_ref, a_ref, kc_ref, vc_ref, h_scr, q_scr, ka_scr, kb_scr, *, b0, ln_rows, qt, unroll=1):
    seq, d = x_ref.shape
    width = a_ref.shape[-1]
    n_heads = width // hd
    length = lens_ref[pl.program_id(0) + b0]

    @pl.loop(0, seq // ln_rows, unroll=unroll)
    def _(r):
        rows = pl.ds(pl.multiple_of(r * ln_rows, ln_rows), ln_rows)
        x = x_ref[rows, :].astype(F32)
        mu = jnp.mean(x, axis=-1, keepdims=True)
        c = x - mu
        var = jnp.mean(c * c, axis=-1, keepdims=True)
        h_scr[rows, :] = (c * lax.rsqrt(var + 1e-5) * g_ref[...] + bt_ref[...]).astype(BF16)

    q = lax.dot_general(h_scr[...], wt_ref[:width, :], NT, preferred_element_type=F32)
    q_scr[...] = (q + bq_ref[...]).astype(BF16)
    keep = lax.broadcasted_iota(jnp.int32, (width, seq), 1) < length
    kt = lax.dot_general(wt_ref[width:2 * width, :], h_scr[...], NT, preferred_element_type=F32)
    kt = jnp.where(keep, kt + bkv_ref[:width, :], 0.0).astype(BF16)
    kc_ref[...] = kt
    row = lax.broadcasted_iota(jnp.int32, (width, seq), 0)
    bias = jnp.where(keep, 0.0, -1e30).astype(BF16)
    ka_scr[...] = jnp.where(row == width - 1, bias, kt)
    kb_scr[...] = jnp.where(row == 0, bias, kt)
    vt = lax.dot_general(wt_ref[2 * width:, :], h_scr[...], NT, preferred_element_type=F32)
    vc_ref[...] = jnp.where(keep, vt + bkv_ref[width:, :], 0.0).astype(BF16)

    c2 = hd ** -0.5 * math.log2(math.e)
    lane = lax.broadcasted_iota(jnp.int32, (qt, width), 1)
    causal = lax.broadcasted_iota(jnp.int32, (qt, qt), 1) <= lax.broadcasted_iota(jnp.int32, (qt, qt), 0)
    for i in range(seq // qt):
        span = (i + 1) * qt
        q_tile = q_scr[i * qt:(i + 1) * qt, :]
        out = jnp.zeros((qt, width), F32)
        for h in range(n_heads):
            low = h < n_heads // 2
            mine = (lane >= h * hd) & (lane < (h + 1) * hd)
            flag = lane == (width - 1 if low else 0)
            qm = jnp.where(mine, q_tile, jnp.where(flag, 1.0, 0.0).astype(BF16))
            k_src = ka_scr if low else kb_scr
            s = jnp.dot(qm, k_src[:, :span], preferred_element_type=F32)
            s_diag = jnp.where(causal, s[:, span - qt:], -1e30)
            s = jnp.concatenate([s[:, :span - qt], s_diag], axis=1) if i else s_diag
            m = jnp.max(s, axis=-1, keepdims=True)
            p = jnp.exp2((s - m) * c2)
            l = jnp.sum(p, axis=-1, keepdims=True)
            p = (p * (1.0 / l)).astype(BF16)
            pv = lax.dot_general(p, vc_ref[:, :span], NT, preferred_element_type=F32)
            out = jnp.where(mine, pv, out)
        a_ref[i * qt:(i + 1) * qt, :] = out.astype(BF16)

def k1(x_in, seq_lens, g, bt, w_qkv, b_qkv, *, ln_rows=64, qt=256, unroll=1, vmem=60 * 2**20):
    nb, seq, d = x_in.shape
    _, _, nh, hd = w_qkv.shape
    width = nh * hd
    wt = jnp.transpose(w_qkv, (1, 2, 3, 0)).reshape(3 * width, d)
    bq = b_qkv.astype(F32).reshape(3, width)
    full = lambda *shape: pl.BlockSpec(shape, lambda b, lens: (0,) * len(shape))
    per = lambda *shape: pl.BlockSpec((None,) + shape, lambda b, lens: (b,) + (0,) * len(shape))
    a, kc, vc = pl.pallas_call(
        functools.partial(k1_body, hd, b0=0, ln_rows=ln_rows, qt=qt, unroll=unroll),
        out_shape=[jax.ShapeDtypeStruct((nb, seq, width), BF16)] + [jax.ShapeDtypeStruct((nb, width, seq), BF16)] * 2,
        grid_spec=pltpu.PrefetchScalarGridSpec(
            num_scalar_prefetch=1, grid=(nb,),
            in_specs=[per(seq, d), full(1, d), full(1, d), full(3 * width, d), full(1, width), full(2 * width, 1)],
            out_specs=[per(seq, width), per(width, seq), per(width, seq)],
            scratch_shapes=[pltpu.VMEM((seq, d), BF16), pltpu.VMEM((seq, width), BF16), pltpu.VMEM((width, seq), BF16), pltpu.VMEM((width, seq), BF16)],
        ),
        compiler_params=pltpu.CompilerParams(vmem_limit_bytes=vmem),
        cost_estimate=pl.CostEstimate(flops=2 * nb * seq * d * 3 * width + 2 * nb * seq * seq * width, bytes_accessed=2 * nb * seq * (d + 3 * width), transcendentals=nb * nh * seq * seq // 2),
    )(seq_lens, x_in, g.reshape(1, d), bt.reshape(1, d), wt, bq[:1], bq[1:].reshape(2 * width, 1))
    un = lambda t: jnp.transpose(t.reshape(nb, nh, hd, seq), (0, 1, 3, 2))
    return a, un(kc), un(vc)

def k2_body(n, a_ref, x_ref, wu_in, wd_in, wo_in, flu, fld, flo, fru, frd, fro, bup_ref, g_ref, bt_ref, bo_ref, bd_ref,
            out_ref, aall, wu, wd, wo,
            acc, h2, stage, ubuf, wub, wdb, abuf, wob, bups,
            send_sems, recv_sems, sem_u, sem_d, sem_a, sem_o, sem_x, sem_g):
    nb, seq, d = x_ref.shape
    ff = wu_in.shape[1]
    width = a_ref.shape[-1]
    rb = seq // n
    hb = nb // 2
    half_rows = hb * rb
    me = lax.axis_index("tp")
    dp = lax.axis_index("dp")
    par = lax.rem(dp, 2)
    core = lax.rem(me, 2)
    flip = 1 - 2 * core
    rgt, lft, opp = lax.rem(me + 2, n), lax.rem(me + n - 2, n), lax.rem(me + n // 2, n)
    sib, lft2, rgt2, opp2 = me + flip, lft + flip, rgt + flip, opp + flip
    to_r, to_l, to_s = {"tp": rgt}, {"tp": lft}, {"tp": sib}
    to_p = {"dp": dp + 1 - 2 * par}

    count = [0]
    copies, got = [], set()

    def remote(src, dst, target):
        i = count[0]
        count[0] += 1
        c = pltpu.make_async_remote_copy(src_ref=src, dst_ref=dst, send_sem=send_sems.at[i], recv_sem=recv_sems.at[i], device_id=target, device_id_type=pl.DeviceIdType.MESH)
        c.start()
        copies.append(c)
        return c

    def ensure(*cs):
        for c in cs:
            if id(c) not in got:
                got.add(id(c))
                c.wait_recv()

    barrier = pltpu.get_barrier_semaphore()
    for r in range(1, n):
        pl.semaphore_signal(barrier, inc=1, device_id={"tp": lax.rem(me + r, n)}, device_id_type=pl.DeviceIdType.MESH)
    pl.semaphore_signal(barrier, inc=1, device_id=to_p, device_id_type=pl.DeviceIdType.MESH)
    pl.semaphore_wait(barrier, n)

    ku, kd, ko = d // 2, ff // 2, width
    qu, qd = d // 4, ff // 4
    cu, cd = pl.multiple_of(ku + par * qu, qu), pl.multiple_of(kd + par * qd, qd)
    eu, ed = pl.multiple_of(ku + (1 - par) * qu, qu), pl.multiple_of(kd + (1 - par) * qd, qd)

    def x_copy(h):
        rows = pl.ds(pl.multiple_of(me * rb, rb), rb)
        return pltpu.make_async_copy(x_ref.at[h * hb:(h + 1) * hb, rows, :], stage.at[h], sem_x.at[h])
    x_copies = [x_copy(0), x_copy(1)]
    x_copies[0].start()

    a2a = {}
    def send_a(h):
        for r in (2, n - 2, 3, n - 3, 4, 5, 1) if n == 8 else range(1, n):
            pass
        for r in sorted(range(1, n)):
            t = lax.rem(me + r, n)
            a2a[h, r] = remote(a_ref.at[h * hb:(h + 1) * hb, pl.ds(pl.multiple_of(t * rb, rb), rb), :], aall.at[h, me], {"tp": t})
    send_a(0)
    bup = [remote(bup_ref, bups.at[me], {"tp": lax.rem(me + r, n)}) for r in range(1, n)]
    bups[me] = bup_ref[...]
    s_wo = remote(wo_in, wo.at[me], to_s)
    s_lo = remote(flo, wo.at[lft], to_s)
    s_ro = remote(fro, wo.at[rgt], to_s)
    f_o = [remote(flo.at[:ko // 2], wo.at[lft, :ko // 2], to_r), remote(fro.at[ko // 2:], wo.at[rgt, ko // 2:], to_l)]
    p_lu = remote(flu.at[ku:], wu.at[lft, pl.ds(cu, qu)], to_p)
    p_ld = remote(fld.at[kd:], wd.at[lft, pl.ds(cd, qd)], to_p)
    p_ru = remote(fru.at[ku:], wu.at[rgt, pl.ds(cu, qu)], to_p)
    p_rd = remote(frd.at[kd:], wd.at[rgt, pl.ds(cd, qd)], to_p)
    f_cu = [remote(flu.at[ku:ku + qu // 2], wu.at[lft, pl.ds(cu, qu // 2)], to_r),
            remote(fru.at[ku + qu // 2:], wu.at[rgt, pl.ds(cu + qu // 2, qu // 2)], to_l)]
    f_cd = [remote(fld.at[kd:kd + qd // 2], wd.at[lft, pl.ds(cd, qd // 2)], to_r),
            remote(frd.at[kd + qd // 2:], wd.at[rgt, pl.ds(cd + qd // 2, qd // 2)], to_l)]
    send_a(1)
    f_uu = [remote(flu.at[:ku // 2], wu.at[lft, :ku // 2], to_r), remote(fru.at[ku // 2:ku], wu.at[rgt, ku // 2:ku], to_l)]
    f_ud = [remote(fld.at[:kd // 2], wd.at[lft, :kd // 2], to_r), remote(frd.at[kd // 2:kd], wd.at[rgt, kd // 2:kd], to_l)]
    s_own = [remote(wu_in, wu.at[me], to_s), remote(wd_in, wd.at[me], to_s)]
    s_l = [remote(flu.at[:ku], wu.at[lft, :ku], to_s), remote(flu.at[ku:], wu.at[lft, pl.ds(cu, qu)], to_s),
           remote(fld.at[:kd], wd.at[lft, :kd], to_s), remote(fld.at[kd:], wd.at[lft, pl.ds(cd, qd)], to_s)]
    s_r = [remote(fru.at[:ku], wu.at[rgt, :ku], to_s), remote(fru.at[ku:], wu.at[rgt, pl.ds(cu, qu)], to_s),
           remote(frd.at[:kd], wd.at[rgt, :kd], to_s), remote(frd.at[kd:], wd.at[rgt, pl.ds(cd, qd)], to_s)]
    x_copies[1].start()

    done = {}
    def on_pair(name, slot, cu_copy, cd_copy):
        if name in done:
            return
        ensure(cu_copy)
        one = remote(wu.at[slot, pl.ds(eu, qu)], wu.at[slot, pl.ds(eu, qu)], to_s)
        ensure(cd_copy)
        done[name] = [one, remote(wd.at[slot, pl.ds(ed, qd)], wd.at[slot, pl.ds(ed, qd)], to_s)]
    def on_opp_o():
        ensure(*f_o)
        done["opp_o"] = [remote(wo.at[opp], wo.at[opp], to_s)]
    def on_opp_c():
        ensure(*f_cu)
        done["p_ou"] = remote(wu.at[opp, pl.ds(cu, qu)], wu.at[opp, pl.ds(cu, qu)], to_p)
        s1 = remote(wu.at[opp, pl.ds(cu, qu)], wu.at[opp, pl.ds(cu, qu)], to_s)
        ensure(*f_cd)
        done["p_od"] = remote(wd.at[opp, pl.ds(cd, qd)], wd.at[opp, pl.ds(cd, qd)], to_p)
        done["opp_c"] = [s1, remote(wd.at[opp, pl.ds(cd, qd)], wd.at[opp, pl.ds(cd, qd)], to_s)]
    def on_opp_u():
        ensure(*f_uu)
        s1 = remote(wu.at[opp, :ku], wu.at[opp, :ku], to_s)
        ensure(*f_ud)
        done["opp_u"] = [s1, remote(wd.at[opp, :kd], wd.at[opp, :kd], to_s)]
    ev_pair_l = lambda: on_pair("pair_l", lft, p_lu, p_ld)
    ev_pair_r = lambda: on_pair("pair_r", rgt, p_ru, p_rd)
    ev_pair_o = lambda: on_pair("pair_o", opp, done["p_ou"], done["p_od"])

    def load(place, slot):
        u, dn = wub.at[slot], wdb.at[slot]
        if place == "own":
            parts = [(wu_in, u, sem_u), (wd_in, dn, sem_d)]
        elif place in ("lft", "rgt"):
            fu, fd, at = (flu, fld, lft) if place == "lft" else (fru, frd, rgt)
            ensure(*((p_lu, p_ld) if place == "lft" else (p_ru, p_rd)))
            parts = [(fu.at[:ku], u.at[:ku], sem_u), (fu.at[ku:], u.at[pl.ds(cu, qu)], sem_u), (wu.at[at, pl.ds(eu, qu)], u.at[pl.ds(eu, qu)], sem_u),
                     (fd.at[:kd], dn.at[:kd], sem_d), (fd.at[kd:], dn.at[pl.ds(cd, qd)], sem_d), (wd.at[at, pl.ds(ed, qd)], dn.at[pl.ds(ed, qd)], sem_d)]
        else:
            need = {"sib": s_own, "lft2": s_l + done.get("pair_l", []), "rgt2": s_r + done.get("pair_r", []), "opp": [], "opp2": []}[place]
            if place == "opp":
                need = f_uu + f_ud + f_cu + f_cd + [done["p_ou"], done["p_od"]]
            if place == "opp2":
                need = done["opp_c"] + done["opp_u"] + done["pair_o"]
            ensure(*need)
            at = {"sib": sib, "lft2": lft2, "rgt2": rgt2, "opp": opp, "opp2": opp2}[place]
            parts = [(wu.at[at], u, sem_u), (wd.at[at], dn, sem_d)]
        for src, dst, sem in parts:
            pltpu.make_async_copy(src, dst, sem.at[slot]).start()

    idx = {"own": me, "sib": sib, "lft": lft, "lft2": lft2, "rgt": rgt, "rgt2": rgt2, "opp": opp, "opp2": opp2}
    tile = 256

    def mlp(h, place, slot):
        pltpu.make_async_copy(wu.at[0], wub.at[slot], sem_u.at[slot]).wait()
        at = idx[place]
        @pl.loop(0, ff // tile)
        def _(i):
            cols = pl.ds(pl.multiple_of(i * tile, tile), tile)
            u = jnp.dot(h2[h], wub[slot, :, cols], preferred_element_type=F32)
            ubuf[:, cols] = jnp.maximum(u + bups[at, 0:1, cols], 0.0).astype(BF16)
        pltpu.make_async_copy(wd.at[0], wdb.at[slot], sem_d.at[slot]).wait()
        @pl.loop(0, d // tile)
        def _(i):
            cols = pl.ds(pl.multiple_of(i * tile, tile), tile)
            acc[h, :, cols] += jnp.dot(ubuf[...], wdb[slot, :, cols], preferred_element_type=F32)

    def load_a(h):
        rows = pl.ds(pl.multiple_of(me * rb, rb), rb)
        cs = [pltpu.make_async_copy(a_ref.at[h * hb:(h + 1) * hb, rows, :], abuf.at[:, :, pl.ds(pl.multiple_of(me * width, width), width)], sem_a.at[0])]
        cs[0].start()
        for r in range(1, n):
            ensure(a2a[h, r])
            j = lax.rem(me + n - r, n)
            c = pltpu.make_async_copy(aall.at[h, j], abuf.at[:, :, pl.ds(pl.multiple_of(j * width, width), width)], sem_a.at[r])
            c.start()
            cs.append(c)
        for c in cs:
            c.wait()

    def proj(h):
        x_copies[h].wait()
        @pl.loop(0, d // tile)
        def _(i):
            cols = pl.ds(pl.multiple_of(i * tile, tile), tile)
            o = jnp.dot(abuf[...].reshape(half_rows, n * width), wob[:, cols], preferred_element_type=F32)
            acc[h, :, cols] = o
        @pl.loop(0, hb)
        def _(b):
            rows = pl.ds(pl.multiple_of(b * rb, rb), rb)
            x1 = (stage[h, b].astype(F32) + acc[h, rows, :] + bo_ref[...]).astype(BF16).astype(F32)
            mu = jnp.mean(x1, axis=-1, keepdims=True)
            c = x1 - mu
            var = jnp.mean(c * c, axis=-1, keepdims=True)
            h2[h, rows, :] = (c * lax.rsqrt(var + 1e-5) * g_ref[...] + bt_ref[...]).astype(BF16)
            acc[h, rows, :] = x1 + bd_ref[...]

    def put_o(src, j, i):
        c = pltpu.make_async_copy(src, wob.at[pl.ds(pl.multiple_of(j * width, width), width)], sem_o.at[i])
        c.start()
        return c
    oc = [put_o(wo_in, me, 0), put_o(flo, lft, 1), put_o(fro, rgt, 2)]
    load("own", 0)
    ensure(s_wo); oc.append(put_o(wo.at[sib], sib, 3))
    ensure(s_lo); oc.append(put_o(wo.at[lft2], lft2, 4))
    ensure(s_ro); oc.append(put_o(wo.at[rgt2], rgt2, 5))
    load("sib", 1)
    ensure(*bup)
    on_opp_o()
    oc.append(put_o(wo.at[opp], opp, 6))
    load_a(0)
    ensure(*done["opp_o"]); oc.append(put_o(wo.at[opp2], opp2, 7))
    for c in oc:
        c.wait()
    proj(0)

    out_own = {}
    def finish(h):
        rows = pl.ds(pl.multiple_of(me * rb, rb), rb)
        for b in range(hb):
            stage[h, b] = acc[h, b * rb:(b + 1) * rb, :].astype(BF16)
        cut = hb // 2
        right = list(range(hb))
        left = right[cut:] + right[:cut]
        loc = pltpu.make_async_copy(stage.at[h], out_ref.at[h * hb:(h + 1) * hb, rows, :], sem_g.at[h])
        loc.start()
        for b1, b2 in zip(right, left):
            for b, to, key in ((b1, to_r, "r"), (b2, to_l, "l")):
                out_own[h, b, key] = remote(stage.at[h, b], out_ref.at[h * hb + b, rows, :], to)
        for b in range(hb):
            out_own[h, b, "s"] = remote(stage.at[h, b], out_ref.at[h * hb + b, rows, :], to_s)
        return loc

    fwd, sdone = {}, []
    def at_out(h, b, owner):
        return out_ref.at[h * hb + b, pl.ds(pl.multiple_of(owner * rb, rb), rb), :]
    def pass_on(h, b, key):
        owner, onward = (lft, to_r) if key == "r" else (rgt, to_l)
        ensure(out_own[h, b, key])
        if (b < hb // 2) == (key == "r"):
            fwd[h, b] = remote(at_out(h, b, owner), at_out(h, b, owner), onward)
        sdone.append(remote(at_out(h, b, owner), at_out(h, b, owner), to_s))
    def last(h, b):
        ensure(fwd[h, b])
        sdone.append(remote(at_out(h, b, opp), at_out(h, b, opp), to_s))

    tasks = [(0, "own"), (0, "sib"), (0, "lft"), (0, "lft2"), "proj1", (1, "own"), (1, "sib"), (1, "lft"), (1, "lft2"),
             (0, "rgt"), (0, "rgt2"), (1, "rgt"), (1, "rgt2"), (0, "opp"), (0, "opp2"), "fin0", (1, "opp"), "xo", (1, "opp2"), "fin1"]
    late = {(0, "lft"): [ev_pair_l], (0, "lft2"): [], (0, "rgt"): [on_opp_c, ev_pair_r], (0, "rgt2"): [], (0, "opp"): [ev_pair_o, on_opp_u], (0, "opp2"): []}
    slot = 0
    loaded = {0: (0, "own"), 1: (0, "sib")}
    order = [t for t in tasks if isinstance(t, tuple)]
    where = {order[0]: 0, order[1]: 1}
    nxt = 2
    locs = []
    def run_late(t):
        for e in late.get(t, []):
            e()
    def fetch(pos, s):
        t = order[pos]
        run_late(t)
        load(t[1], s)
        where[t] = s
    pos = 0
    for t in tasks:
        if t == "proj1":
            load_a(1)
            proj(1)
        elif t in ("fin0", "fin1"):
            locs.append(finish(int(t[-1])))
        elif t == "xo":
            pass_on(0, 0, "r")
            pass_on(0, hb // 2, "l")
        else:
            if t not in where:
                fetch(pos, pos % 2)
            mlp(t[0], t[1], where[t])
            if pos + 2 < len(order):
                nt = order[pos + 2]
                if nt not in late:
                    fetch(pos + 2, pos % 2)
            pos += 1
    cut = hb // 2
    for h in (0, 1):
        for i in range(cut):
            if (h, i) != (0, 0):
                pass_on(h, i, "r")
                pass_on(h, cut + i, "l")
        for i in range(cut):
            pass_on(h, cut + i, "r")
            pass_on(h, i, "l")
        if h == 1:
            for i in range(cut):
                last(0, i); last(0, cut + i)
    for i in range(cut):
        last(1, i); last(1, cut + i)
    for c in locs:
        c.wait()
    ensure(*copies)
    for c in copies:
        c.wait_send()

N_COPIES = 160

def k2(n, a, x_in, w_up, w_down, w_out, fl, fr, b_up, g, bt, b_out, b_down, *, vmem=63 * 2**20, ncopies=N_COPIES, cid=0):
    nb, seq, d = x_in.shape
    ff = w_up.shape[1]
    width = a.shape[-1]
    rb, hb = seq // n, nb // 2
    hr = rb * hb
    any_ = pl.BlockSpec(memory_space=pl.ANY)
    vm = pl.BlockSpec(memory_space=pltpu.VMEM)
    row = lambda t: t.astype(F32).reshape(1, -1)
    sds = jax.ShapeDtypeStruct
    outs = pl.pallas_call(
        functools.partial(k2_body, n),
        out_shape=[sds((nb, seq, d), BF16), sds((2, n, hb, rb, width), BF16), sds((n, d, ff), BF16), sds((n, ff, d), BF16), sds((n, width, d), BF16)],
        in_specs=[any_] * 11 + [vm] * 5,
        out_specs=[any_] * 5,
        scratch_shapes=[
            pltpu.VMEM((2, hr, d), F32), pltpu.VMEM((2, hr, d), BF16), pltpu.VMEM((2, hb, rb, d), BF16), pltpu.VMEM((hr, ff), BF16),
            pltpu.VMEM((2, d, ff), BF16), pltpu.VMEM((2, ff, d), BF16), pltpu.VMEM((hb, rb, n * width), BF16), pltpu.VMEM((n * width, d), BF16),
            pltpu.VMEM((n, 8, ff), F32),
            pltpu.SemaphoreType.DMA((ncopies,)), pltpu.SemaphoreType.DMA((ncopies,)),
            pltpu.SemaphoreType.DMA((2,)), pltpu.SemaphoreType.DMA((2,)), pltpu.SemaphoreType.DMA((n,)), pltpu.SemaphoreType.DMA((n,)),
            pltpu.SemaphoreType.DMA((2,)), pltpu.SemaphoreType.DMA((2,)),
        ],
        compiler_params=pltpu.CompilerParams(collective_id=cid, has_side_effects=True, vmem_limit_bytes=vmem),
        cost_estimate=pl.CostEstimate(flops=2 * nb * rb * d * (4 * ff * n + 2 * n * width) // 2, bytes_accessed=4 * n * d * ff * 2, transcendentals=0),
    )(a, x_in, w_up, w_down, w_out, *fl, *fr, jnp.broadcast_to(row(b_up), (8, ff)), row(g), row(bt), row(b_out), row(b_down))
    return outs[0]

def moved(n, dp_index, w_up, w_down, w_out):
    par = lax.rem(dp_index, 2)
    def block(w):
        q = w.shape[0] // 4
        return jnp.concatenate([w[:2 * q], lax.dynamic_slice_in_dim(w, (2 + par) * q, q, 0)], axis=0)
    parts = (block(w_up), block(w_down), w_out)
    right = [(i, (i + 2) % n) for i in range(n)]
    left = [(i, (i - 2) % n) for i in range(n)]
    fl = [lax.ppermute(t, "tp", right) for t in parts]
    fr = [lax.ppermute(t, "tp", left) for t in parts]
    return fl, fr


def solution(mesh):
    n = mesh.shape["tp"]

    def local_layer(x_in, seq_lens, ln1_gain, ln1_bias, w_qkv, b_qkv, w_out, b_out, ln2_gain, ln2_bias, w_up, b_up, w_down, b_down):
        w_o = w_out.reshape(-1, w_out.shape[-1])
        fl, fr = moved(n, lax.axis_index("dp"), w_up, w_down, w_o)
        a, k_cache, v_cache = k1(x_in, seq_lens, ln1_gain, ln1_bias, w_qkv, b_qkv, ln_rows=256, unroll=4)
        x_out = k2(n, a, x_in, w_up, w_down, w_o, fl, fr, b_up, ln2_gain, ln2_bias, b_out, b_down)
        return x_out, k_cache, v_cache

    arg_specs = (P("dp", None, None), P("dp"), P(), P(), P(None, None, "tp", None), P(None, "tp", None), P("tp", None, None), P(), P(), P(), P(None, "tp"), P("tp"), P("tp", None), P())
    cache_spec = P("dp", "tp", None, None)
    result_specs = (P("dp", None, None), cache_spec, cache_spec)
    return jax.shard_map(local_layer, mesh=mesh, in_specs=arg_specs, out_specs=result_specs, check_vma=False)
```

```python
import functools
import math

import jax
import jax.numpy as jnp
from jax import lax
from jax.experimental import pallas as pl
from jax.experimental.pallas import tpu as pltpu
from jax.sharding import PartitionSpec as P

F32 = jnp.float32
BF16 = jnp.bfloat16
NT = (((1,), (1,)), ((), ()))
MESH = pl.DeviceIdType.MESH


def norm(x, gain, bias):
    mu = jnp.mean(x, axis=-1, keepdims=True)
    c = x - mu
    var = jnp.mean(c * c, axis=-1, keepdims=True)
    return (c * lax.rsqrt(var + 1e-5) * gain + bias).astype(BF16)


def attention_rows(hd, qt, length, x_ref, h_scr, wt_ref, g_ref, bt_ref, bq_ref, bkv_ref, a_ref, kv_ref, q_scr, ka_scr, kb_scr):
    seq, width = a_ref.shape
    n_heads = width // hd
    rows = seq // 4
    for r in range(4):
        h_scr[r * rows:(r + 1) * rows, :] = norm(x_ref[r * rows:(r + 1) * rows, :].astype(F32), g_ref[...], bt_ref[...])
    q = lax.dot_general(h_scr[...], wt_ref[:width, :], NT, preferred_element_type=F32)
    q_scr[...] = (q + bq_ref[...]).astype(BF16)
    keep = lax.broadcasted_iota(jnp.int32, (width, seq), 1) < length
    kt = lax.dot_general(wt_ref[width:2 * width, :], h_scr[...], NT, preferred_element_type=F32)
    kt = jnp.where(keep, kt + bkv_ref[:width, :], 0.0).astype(BF16)
    kv_ref[:width, :] = kt
    row = lax.broadcasted_iota(jnp.int32, (width, seq), 0)
    bias = jnp.where(keep, 0.0, -1e30).astype(BF16)
    ka_scr[...] = jnp.where(row == width - 1, bias, kt)
    kb_scr[...] = jnp.where(row == 0, bias, kt)
    vt = lax.dot_general(wt_ref[2 * width:, :], h_scr[...], NT, preferred_element_type=F32)
    kv_ref[width:, :] = jnp.where(keep, vt + bkv_ref[width:, :], 0.0).astype(BF16)

    c2 = hd ** -0.5 * math.log2(math.e)
    lane = lax.broadcasted_iota(jnp.int32, (qt, width), 1)
    causal = lax.broadcasted_iota(jnp.int32, (qt, qt), 1) <= lax.broadcasted_iota(jnp.int32, (qt, qt), 0)
    for i in range(seq // qt):
        span = (i + 1) * qt
        q_tile = q_scr[i * qt:(i + 1) * qt, :]
        out = jnp.zeros((qt, width), F32)
        for h in range(n_heads):
            low = h < n_heads // 2
            mine = (lane >= h * hd) & (lane < (h + 1) * hd)
            flag = lane == (width - 1 if low else 0)
            qm = jnp.where(mine, q_tile, jnp.where(flag, 1.0, 0.0).astype(BF16))
            k_src = ka_scr if low else kb_scr
            s = jnp.dot(qm, k_src[:, :span], preferred_element_type=F32)
            s_diag = jnp.where(causal, s[:, span - qt:], -1e30)
            s = jnp.concatenate([s[:, :span - qt], s_diag], axis=1) if i else s_diag
            m = jnp.max(s, axis=-1, keepdims=True)
            p = jnp.exp2((s - m) * c2)
            total = jnp.sum(p, axis=-1, keepdims=True)
            p = (p * (1.0 / total)).astype(BF16)
            pv = lax.dot_general(p, kv_ref[width:, :span], NT, preferred_element_type=F32)
            out = jnp.where(mine, pv, out)
        a_ref[i * qt:(i + 1) * qt, :] = out.astype(BF16)


def layer_body(n, hd, lens_ref, x_ref, wt_in, wu_in, wd_in, wo_in, bias_ref, g1_ref, t1_ref, g2_ref, t2_ref,
               out_ref, a_hbm, kc_hbm, vc_hbm, aall, wu, wd, wo,
               acc, h2, stage, ubuf, wub, wdb, abuf, wob, bups, bkv_ref, q_scr, ka_scr, kb_scr, ao, kvo,
               send_sems, recv_sems, sem_u, sem_d, sem_a, sem_o, sem_x, sem_k, sem_g, sem_w):
    nb, seq, d = x_ref.shape
    ff = wu_in.shape[1]
    width = wo_in.shape[0]
    rb = seq // n
    hb = nb // 2
    hr = hb * rb
    bo_ref, bd_ref = bias_ref.at[:, :d], bias_ref.at[:, d:2 * d]
    bq_ref = bias_ref.at[:, 2 * d + ff:2 * d + ff + width]
    me = lax.axis_index("tp")
    dp = lax.axis_index("dp")
    par = lax.rem(dp, 2)
    flip = 1 - 2 * lax.rem(me, 2)
    rgt, lft, opp = lax.rem(me + 2, n), lax.rem(me + n - 2, n), lax.rem(me + n // 2, n)
    sib, lft2, rgt2, opp2 = me + flip, lft + flip, rgt + flip, opp + flip
    to_r, to_l, to_s = {"tp": rgt}, {"tp": lft}, {"tp": sib}
    to_p = {"dp": dp + 1 - 2 * par}
    scope = jax.named_scope

    barrier = pltpu.get_barrier_semaphore()
    for r in range(1, n):
        pl.semaphore_signal(barrier, inc=1, device_id={"tp": lax.rem(me + r, n)}, device_id_type=MESH)
    pl.semaphore_signal(barrier, inc=1, device_id=to_p, device_id_type=MESH)
    pl.semaphore_wait(barrier, n)

    copies, got = [], set()

    def remote(src, dst, target):
        i = len(copies)
        c = pltpu.make_async_remote_copy(src_ref=src, dst_ref=dst, send_sem=send_sems.at[i], recv_sem=recv_sems.at[i], device_id=target, device_id_type=MESH)
        copies.append(c)
        return c

    def pieces(ref, names, target, at=None):
        pass

    def start(*cs):
        for c in cs:
            c.start()

    def ensure(*cs):
        for c in cs:
            if id(c) not in got:
                got.add(id(c))
                c.wait_recv()

    uw, cw = ff // 4, 3 * ff // 8
    pc, qc = pl.multiple_of(uw + par * cw, 128), pl.multiple_of(uw + (1 - par) * cw, 128)
    po, qo = pl.multiple_of(par * (width // 2), width // 2), pl.multiple_of((1 - par) * (width // 2), width // 2)
    dh = d // 2
    ua, ub = pl.ds(0, uw // 2), pl.ds(uw // 2, uw // 2)
    part_cols = {"u": pl.ds(0, uw), "p": pl.ds(pc, cw), "q": pl.ds(qc, cw)}
    rows_of = {"": pl.ds(0, d), "a": pl.ds(0, dh), "b": pl.ds(dh, dh)}

    def down_rows(share, half):
        base, size = {"u": (0, uw), "p": (pc, cw), "q": (qc, cw)}[share]
        if half == "":
            return pl.ds(base, size)
        off = base + (size // 2 if half == "b" else 0)
        return pl.ds(off if share == "u" else pl.multiple_of(off, 64), size // 2)

    def out_rows(share, half):
        base, size = {"p": po, "q": qo}[share], width // 2
        if half == "":
            return pl.ds(base, size)
        return pl.ds(pl.multiple_of(base + (size // 2 if half == "b" else 0), size // 2), size // 2)

    def view(kind, slot, share, half):
        if kind == "up":
            ref = wu_in if slot is None else wu.at[slot]
            return ref.at[rows_of[half], part_cols[share]]
        if kind == "dn":
            ref = wd_in if slot is None else wd.at[slot]
            return ref.at[down_rows(share, half), :]
        ref = wo_in if slot is None else wo.at[slot]
        return ref.at[out_rows(share, half), :]

    own, fwd, pair, sb = {}, {}, {}, {}
    halves = [("up", "p"), ("dn", "p"), ("up", "u"), ("dn", "u")]
    for side, target in (("R", to_r), ("L", to_l)):
        own[side, "wo", "p", ""] = remote(view("wo", None, "p", ""), view("wo", me, "p", ""), target)
        for kind, share in halves:
            for half in "ab":
                own[side, kind, share, half] = remote(view(kind, None, share, half), view(kind, me, share, half), target)
    for side, target, half, held in (("R", to_r, "a", lft), ("L", to_l, "b", rgt)):
        for kind, share in [("wo", "p")] + halves:
            fwd[side, kind, share] = remote(view(kind, held, share, half), view(kind, held, share, half), target)
    for name, held in (("lft", lft), ("rgt", rgt), ("opp", opp)):
        pair[name, "wo", ""] = remote(view("wo", held, "p", ""), view("wo", held, "p", ""), to_p)
        for kind in ("up", "dn"):
            for half in "ab":
                pair[name, kind, half] = remote(view(kind, held, "p", half), view(kind, held, "p", half), to_p)
        for kind, share in [("wo", "p"), ("wo", "q"), ("up", "p"), ("up", "q"), ("dn", "p"), ("dn", "q"), ("up", "u"), ("dn", "u")]:
            sb[name, kind, share] = remote(view(kind, held, share, ""), view(kind, held, share, ""), to_s)
    sb["own", "wo"] = remote(wo_in, wo.at[me], to_s)
    sb["own", "up"] = remote(wu_in, wu.at[me], to_s)
    sb["own", "dn"] = remote(wd_in, wd.at[me], to_s)
    bup = [remote(bups.at[me], bups.at[me], {"tp": lax.rem(me + r, n)}) for r in range(1, n)]
    a2a = {}
    for h in (0, 1):
        for r, t in enumerate((sib, rgt, lft, rgt2, lft2, opp, opp2)):
            a2a[h, r] = remote(a_hbm.at[h * hb:(h + 1) * hb, pl.ds(pl.multiple_of(t * rb, rb), rb), :], aall.at[h, me], {"tp": t})

    def at_out(h, b, owner):
        return out_ref.at[h * hb + b, pl.ds(pl.multiple_of(owner * rb, rb), rb), :]
    cut = hb // 2
    first = list(range(hb))
    other = first[cut:] + first[:cut]
    xo, xf, xs = {}, {}, {}
    for h in (0, 1):
        for b in range(hb):
            for side, target in (("R", to_r), ("L", to_l), ("S", to_s)):
                xo[h, b, side] = remote(stage.at[h, b], at_out(h, b, me), target)
            held, target = (lft, to_r) if b < cut else (rgt, to_l)
            xf[h, b] = remote(at_out(h, b, held), at_out(h, b, held), target)
            for name, held in (("lft", lft), ("rgt", rgt), ("opp", opp)):
                xs[h, b, name] = remote(at_out(h, b, held), at_out(h, b, held), to_s)

    src_of = {"lft": "R", "rgt": "L"}

    def got_wo():
        ensure(own["R", "wo", "p", ""], own["L", "wo", "p", ""])
        start(pair["lft", "wo", ""], pair["rgt", "wo", ""], fwd["R", "wo", "p"], fwd["L", "wo", "p"], sb["lft", "wo", "p"], sb["rgt", "wo", "p"])

    def got_first(kind):
        ensure(own["R", kind, "p", "a"], own["L", kind, "p", "b"])
        start(fwd["R", kind, "p"], fwd["L", kind, "p"], pair["lft", kind, "a"])
        if kind == "up":
            start(pair["rgt", kind, "b"])

    def got_second(kind):
        ensure(own["R", kind, "p", "b"], own["L", kind, "p", "a"])
        start(pair["lft", kind, "b"])
        if kind == "dn":
            start(pair["rgt", kind, "b"])
        start(pair["rgt", kind, "a"], sb["lft", kind, "p"], sb["rgt", kind, "p"])

    def got_opp(kind):
        ensure(fwd["R", kind, "p"], fwd["L", kind, "p"])
        if kind == "wo":
            start(pair["opp", "wo", ""])
        else:
            start(pair["opp", kind, "a"], pair["opp", kind, "b"])
        start(sb["opp", kind, "p"])

    def got_pair(name, kind):
        ensure(*[pair[name, kind, half] for half in ([""] if kind == "wo" else "ab")])
        start(sb[name, kind, "q"])

    def got_u(kind):
        ensure(own["R", kind, "u", "a"], own["L", kind, "u", "b"])
        start(fwd["R", kind, "u"], fwd["L", kind, "u"])
        ensure(own["R", kind, "u", "b"], own["L", kind, "u", "a"])
        start(sb["lft", kind, "u"], sb["rgt", kind, "u"])

    def got_opp_u(kind):
        ensure(fwd["R", kind, "u"], fwd["L", kind, "u"])
        start(sb["opp", kind, "u"])

    def send_own(kind, share):
        start(own["R", kind, share, "a"], own["L", kind, share, "b"], own["R", kind, share, "b"], own["L", kind, share, "a"])

    start(own["R", "wo", "p", ""], own["L", "wo", "p", ""])
    send_own("up", "p")
    wt_copy = pltpu.make_async_copy(wt_in, abuf, sem_w.at[0])
    wt_copy.start()

    def x_copy(b, slot):
        return pltpu.make_async_copy(x_ref.at[b], wdb.at[slot], sem_x.at[slot])
    x_copy(0, 0).start()
    start(sb["own", "wo"], sb["own", "up"], sb["own", "dn"])
    bups[me] = jnp.broadcast_to(bias_ref[:, 2 * d:2 * d + ff], (8, ff))
    bkv_ref[...] = jnp.transpose(jnp.broadcast_to(bias_ref[:, 2 * d + ff + width:], (8, 2 * width)))[:, :1]
    my_rows = pl.ds(pl.multiple_of(me * rb, rb), rb)
    own_x = [pltpu.make_async_copy(x_ref.at[h * hb:(h + 1) * hb, my_rows, :], stage.at[h], sem_g.at[h]) for h in (0, 1)]
    wt_copy.wait()

    def put_outs(b, slot):
        return [pltpu.make_async_copy(ao.at[slot], a_hbm.at[b], sem_k.at[slot, 0]), pltpu.make_async_copy(kvo.at[slot, :width], kc_hbm.at[b], sem_k.at[slot, 1]),
                pltpu.make_async_copy(kvo.at[slot, width:], vc_hbm.at[b], sem_k.at[slot, 2])]

    def wo_load(j, i):
        src = wo_in if i == 0 else wo.at[j]
        return pltpu.make_async_copy(src, wob.at[pl.ds(pl.multiple_of(j * width, width), width)], sem_o.at[i])
    wo_loads = [wo_load(j, i) for i, j in enumerate((me, sib, lft, lft2, rgt, rgt2, opp, opp2))]

    def early():
        wo_loads[0].start()
        start(*bup)
        start(*own_x)

    def near_wo():
        got_pair("lft", "wo")
        got_pair("rgt", "wo")

    events = {
        0: [got_wo, early],
        2: [lambda: got_first("up"), lambda: send_own("dn", "p")],
        4: [lambda: got_opp("wo"), lambda: got_second("up"), near_wo],
        6: [lambda: start(*[a2a[0, r] for r in range(n - 1)]), lambda: got_opp("up")],
        7: [lambda: got_first("dn"), lambda: send_own("up", "u"), lambda: send_own("dn", "u")],
        9: [lambda: got_second("dn"), lambda: got_pair("opp", "wo")],
        11: [lambda: got_pair("lft", "up"), lambda: got_pair("rgt", "up")],
    }

    @pl.loop(0, nb)
    def _(b):
        slot = lax.rem(b, 2)
        x_copy(b, slot).wait()

        @pl.when(b + 1 < nb)
        def _():
            x_copy(b + 1, 1 - slot).start()
        with scope("attention"):
            attention_rows(hd, min(256, seq), lens_ref[b], wdb.at[slot], h2, abuf, g1_ref, t1_ref, bq_ref, bkv_ref, ao.at[slot], kvo.at[slot], q_scr, ka_scr, kb_scr)
        for c in put_outs(b, slot):
            c.start()

        @pl.when(b > 0)
        def _():
            for c in put_outs(b - 1, 1 - slot):
                c.wait()
        for k, todo in events.items():
            @pl.when(b == k)
            def _(k=k, todo=todo):
                with scope("event%d" % k):
                    for e in todo:
                        e()
    for c in put_outs(nb - 1, (nb - 1) % 2):
        c.wait()

    def shard_at(k, other):
        return lax.rem(me + 3 * k * (k + 1), n) + other * flip

    tile = 256

    def whole(j, slot):
        return [pltpu.make_async_copy(wu.at[j], wub.at[slot], sem_u.at[slot]), pltpu.make_async_copy(wd.at[j], wdb.at[slot], sem_d.at[slot])]

    def own_whole(slot):
        return [pltpu.make_async_copy(wu_in, wub.at[slot], sem_u.at[slot]), pltpu.make_async_copy(wd_in, wdb.at[slot], sem_d.at[slot])]

    def load_shares(j, shares, slot):
        at = 0
        for share in shares:
            size = uw if share == "u" else cw
            pltpu.make_async_copy(view("up", j, share, ""), wub.at[slot, :, at:at + size], sem_u.at[slot]).start()
            pltpu.make_async_copy(view("dn", j, share, ""), wdb.at[slot, at:at + size], sem_d.at[slot]).start()
            at += size

    def mlp(j, shares, slot):
        if shares == "all":
            spans = [(c, slice(c, c + tile), tile) for c in range(0, ff, tile)]
        else:
            spans, at = [], 0
            for share in shares:
                base, size = {"u": (0, uw), "p": (pc, cw), "q": (qc, cw)}[share]
                spans.append((at, pl.ds(base, size), size))
                at += size
        size = sum(w for _, _, w in spans)
        pltpu.make_async_copy(wu.at[0, :, :size], wub.at[slot, :, :size], sem_u.at[slot]).wait()
        for at, cols, w in spans:
            u = jnp.dot(h2[:hr], wub[slot, :, at:at + w], preferred_element_type=F32)
            ubuf[:, at:at + w] = jnp.maximum(u + bups[j, 0:1, cols], 0.0).astype(BF16)
        pltpu.make_async_copy(wd.at[0, :size], wdb.at[slot, :size], sem_d.at[slot]).wait()
        for c in range(0, d, tile):
            acc[:, c:c + tile] += jnp.dot(ubuf[:, :size], wdb[slot, :size, c:c + tile], preferred_element_type=F32)

    def load_a(h):
        def put(src, j, i):
            for b in range(hb):
                c = pltpu.make_async_copy(src.at[b], abuf.at[b * rb:(b + 1) * rb, pl.ds(pl.multiple_of(j * width, width), width)], sem_a.at[i])
                c.start()
                yield c
        cs = list(put(a_hbm.at[h * hb:(h + 1) * hb, my_rows, :], me, 0))
        for r, j in enumerate((sib, lft, rgt, lft2, rgt2, opp, opp2)):
            ensure(a2a[h, r])
            cs += list(put(aall.at[h, j], j, r + 1))
        for i in range(n):
            pltpu.make_async_copy(aall.at[h, i], aall.at[h, i], sem_a.at[i]).wait()

    def proj(h):
        own_x[h].wait() if h == 0 else None
        @pl.loop(0, d // tile, unroll=PROJ_UNROLL)
        def _(i):
            cols = pl.ds(pl.multiple_of(i * tile, tile), tile)
            acc[:, cols] = jnp.dot(abuf[...], wob[:, cols], preferred_element_type=F32)
        @pl.loop(0, hb)
        def _(b):
            rows = pl.ds(pl.multiple_of(b * rb, rb), rb)
            x1 = (stage[h, b].astype(F32) + acc[rows, :] + bo_ref[...]).astype(BF16).astype(F32)
            h2[rows, :] = norm(x1, g2_ref[...], t2_ref[...])
            acc[rows, :] = x1 + bd_ref[...]

    put_own = [pltpu.make_async_copy(stage.at[h], out_ref.at[h * hb:(h + 1) * hb, my_rows, :], sem_g.at[h]) for h in (0, 1)]

    def finish(h):
        for b in range(hb):
            stage[h, b] = acc[b * rb:(b + 1) * rb, :].astype(BF16)
        put_own[h].start()
        for b1, b2 in zip(first, other):
            start(xo[h, b1, "R"], xo[h, b2, "L"])
        start(*[xo[h, b, "S"] for b in range(hb)])

    def pass_on(h, b, side):
        ensure(xo[h, b, side])
        if (b < cut) == (side == "R"):
            start(xf[h, b])
        start(xs[h, b, "lft" if side == "R" else "rgt"])

    def relay(h, i):
        pass_on(h, first[i], "R")
        pass_on(h, other[i], "L")

    def last(h, b):
        ensure(xf[h, b])
        start(xs[h, b, "opp"])

    with scope("wo_loads"):
        ensure(sb["own", "wo"])
        for name in ("lft", "rgt"):
            ensure(sb[name, "wo", "p"], sb[name, "wo", "q"])
        start(*wo_loads[1:6])
        ensure(sb["opp", "wo", "p"], sb["opp", "wo", "q"])
        start(*wo_loads[6:])
        ensure(*bup)
        own_x[1].wait()
    start(*own_whole(0))
    ensure(sb["own", "up"], sb["own", "dn"])
    start(*whole(sib, 1))
    with scope("load_a0"):
        load_a(0)
    with scope("wo_wait"):
        for c in wo_loads:
            c.wait()
    with scope("proj0"):
        proj(0)

    def need(*keys):
        ensure(*[sb[k] for k in keys])

    def sib_keys(name, shares):
        return [(name, kind, share) for kind in ("up", "dn") for share in shares]

    def opposite(shares):
        load_shares(opp, shares, 0)

        @pl.loop(0, 2)
        def _(t):
            @pl.when(t == 0)
            def _():
                need(*sib_keys("opp", shares))
                load_shares(opp2, shares, 1)
            with scope("mlp_" + shares):
                mlp(shard_at(3, t), shares, t)

    def end_of_first_half():
        with scope("arrive_opp_up"):
            got_opp_u("up")
            got_opp_u("dn")
        opposite("pu")
        with scope("arrive_opp_q"):
            got_pair("opp", "dn")
        opposite("q")
        with scope("fin0"):
            finish(0)
        start(*own_whole(0))
        start(*whole(sib, 1))
        with scope("load_a1"):
            load_a(1)
        with scope("proj1"):
            proj(1)

    def arrive_lft():
        got_opp("dn")
        got_pair("opp", "up")
        got_u("up")
        got_u("dn")
        start(*[a2a[1, r] for r in range(n - 1)])
        got_pair("lft", "dn")
        start(*whole(lft, 0))
        need(*sib_keys("lft", "upq"))
        start(*whole(lft2, 1))

    def arrive_rgt():
        got_pair("rgt", "dn")
        start(*whole(rgt, 0))

    def arrive_rgt2():
        need(*sib_keys("rgt", "upq"))
        start(*whole(rgt2, 1))

    steps = n - 2
    first_events = {1: arrive_lft, 3: arrive_rgt, 4: arrive_rgt2, 5: end_of_first_half}

    @pl.loop(0, steps + n)
    def _(s):
        r = s - steps * lax.div(s + n - steps, n)
        slot = lax.rem(s, 2)
        with scope("mlp"):
            mlp(shard_at(lax.div(r, 2), slot), "all", slot)
        for k, event in first_events.items():
            @pl.when(s == k)
            def _(k=k, event=event):
                with scope("first%d" % k):
                    event()
        for k in range(hb):
            @pl.when(s == k + steps + 1)
            def _(k=k):
                with scope("relay0_%d" % k):
                    relay(0, k)

        @pl.when((s >= steps) & (s < steps + n - 2))
        def _():
            start(*whole(shard_at(lax.div(r, 2) + 1, slot), slot))
    with scope("fin1"):
        finish(1)
    for i in range(hb):
        with scope("relay1_%d" % i):
            relay(1, i)
    for h in (0, 1):
        for i in range(cut):
            with scope("last%d_%d" % (h, i)):
                last(h, i)
                last(h, cut + i)
    with scope("final"):
        for h in (0, 1):
            put_own[h].wait()
        ensure(*copies)
        for c in copies:
            c.wait_send()


N_COPIES = 192
PROJ_UNROLL = 2


def layer(n, x_in, seq_lens, g1, t1, w_qkv, b_qkv, w_out, b_out, g2, t2, w_up, b_up, w_down, b_down):
    nb, seq, d = x_in.shape
    _, _, nh, hd = w_qkv.shape
    width = nh * hd
    ff = w_up.shape[1]
    rb, hb = seq // n, nb // 2
    hr = rb * hb
    wt = jnp.transpose(w_qkv, (1, 2, 3, 0)).reshape(3 * width, d)
    bias = jnp.concatenate([t.reshape(1, -1) for t in (b_out, b_down, b_up, b_qkv)], axis=1).astype(F32)
    any_ = pl.BlockSpec(memory_space=pl.ANY)
    vm = pl.BlockSpec(memory_space=pltpu.VMEM)
    row = lambda t: t.astype(F32).reshape(1, -1)
    sds = lambda *shape: jax.ShapeDtypeStruct(shape, BF16)
    dma = lambda *shape: pltpu.SemaphoreType.DMA(shape)
    outs = pl.pallas_call(
        functools.partial(layer_body, n, hd),
        out_shape=[sds(nb, seq, d), sds(nb, seq, width), sds(nb, width, seq), sds(nb, width, seq), sds(2, n, hb, rb, width), sds(n, d, ff), sds(n, ff, d), sds(n, width, d)],
        in_specs=[pl.BlockSpec(memory_space=pltpu.SMEM)] + [any_] * 5 + [vm] * 5,
        out_specs=[any_] * 8,
        scratch_shapes=[
            pltpu.VMEM((hr, d), F32), pltpu.VMEM((seq, d), BF16), pltpu.VMEM((2, hb, rb, d), BF16), pltpu.VMEM((hr, ff), BF16),
            pltpu.VMEM((2, d, ff), BF16), pltpu.VMEM((2, ff, d), BF16), pltpu.VMEM((hr, n * width), BF16), pltpu.VMEM((n * width, d), BF16),
            pltpu.VMEM((n, 8, ff), F32), pltpu.VMEM((2 * width, 1), F32), pltpu.VMEM((seq, width), BF16), pltpu.VMEM((width, seq), BF16), pltpu.VMEM((width, seq), BF16),
            pltpu.VMEM((2, seq, width), BF16), pltpu.VMEM((2, 2 * width, seq), BF16),
            dma(N_COPIES), dma(N_COPIES), dma(2), dma(2), dma(n), dma(n), dma(2), dma(2, 3), dma(2), dma(1),
        ],
        compiler_params=pltpu.CompilerParams(collective_id=0, has_side_effects=True, vmem_limit_bytes=63 * 2**20 + 2**19),
        cost_estimate=pl.CostEstimate(flops=2 * nb * seq * d * 3 * width + nb * rb * d * (4 * ff * n + 2 * n * width), bytes_accessed=8 * n * d * ff, transcendentals=nb * nh * seq * seq // 2),
    )(seq_lens, x_in, wt, w_up, w_down, w_out.reshape(width, d), bias, row(g1), row(t1), row(g2), row(t2))
    un = lambda t: jnp.transpose(t.reshape(nb, nh, hd, seq), (0, 1, 3, 2))
    return outs[0], un(outs[2]), un(outs[3])


def solution(mesh):
    n = mesh.shape["tp"]
    arg_specs = (P("dp", None, None), P("dp"), P(), P(), P(None, None, "tp", None), P(None, "tp", None), P("tp", None, None), P(), P(), P(), P(None, "tp"), P("tp"), P("tp", None), P())
    cache_spec = P("dp", "tp", None, None)
    result_specs = (P("dp", None, None), cache_spec, cache_spec)
    return jax.shard_map(functools.partial(layer, n), mesh=mesh, in_specs=arg_specs, out_specs=result_specs, check_vma=False)
```
